256 devices in a mesh: rep: 1, r: 32 (over y, z), s: 8 (over x, core).
Axes of the slice: x: 4, y: 4, z: 8, core: 2. Of those that a mesh axis runs over, the one named last changes fastest.
Arguments:
- x: bfloat16 [256, 2048, 896], P(('rep', 'r', 's'))
- dy: bfloat16 [256, 2048, 896], P(('rep', 'r', 's'))
- w_gate: bfloat16 [2, 896, 2304], P(None, 's')
- w_up: bfloat16 [2, 896, 2304], P(None, 's')
- w_down: bfloat16 [2, 2304, 896], P(None, 's')
Outputs:
- output 1: bfloat16 [256, 2048, 896], P(('rep', 'r', 's'))
- output 2: bfloat16 [2, 896, 2304], P('rep', 's')
- output 3: bfloat16 [2, 896, 2304], P('rep', 's')
- output 4: bfloat16 [2, 2304, 896], P('rep', 's')
All inputs are finite; a program needn't handle non-finite values.
Results may differ from the reference program's by a relative error of at most 0.018.
Values are sent between devices in bfloat16 or wider.
A program may use at most 768 MiB of HBM per device.

```python
import jax
import jax.numpy as jnp
from jax import lax

SEQUENCES = 256
TOKENS = 2048
D = 896
FF = 2304
LAYERS = 2
NAMES = ("w_gate", "w_up", "w_down")
SHAPES = {"w_gate": (LAYERS, D, FF), "w_up": (LAYERS, D, FF), "w_down": (LAYERS, FF, D)}


def bump(key, n, height):
    away = (jnp.arange(n, dtype=jnp.int32) - jax.random.randint(key, (), 0, n, jnp.int32)) % n
    return jnp.where(away < n // 8, height, 1.0)


def together(key, own, strength):
    shared = jax.random.normal(key, own.shape[1:], jnp.float32)
    return (own + strength * shared) * lax.rsqrt(1 + strength * strength)


def setup_inputs(seed: int = 0, part: int = 0) -> dict:
    kx, kdy, ka, kb, kz, kf, kh, kl, *kw = jax.random.split(jax.random.key(seed), 8 + len(NAMES))
    kx, kdy, ka, kb = (jax.random.fold_in(k, part) for k in (kx, kdy, ka, kb))
    shape = (SEQUENCES, TOKENS, D)
    much_x, much_dy = jax.random.uniform(kz, (2,), jnp.float32, 0.0, 1.0)
    layers = 2.0 ** jax.random.uniform(kl, (LAYERS, 1, 1), jnp.float32, -1.0, 1.0)
    x = together(ka, jax.random.normal(kx, shape, jnp.float32), much_x) * bump(kf, D, 4.0)
    dy = together(kb, jax.random.normal(kdy, shape, jnp.float32), much_dy)
    drawn = {"x": x.astype(jnp.bfloat16), "dy": (dy * (SEQUENCES * TOKENS) ** -0.5).astype(jnp.bfloat16)}
    for key, name in zip(kw, NAMES, strict=True):
        w = jax.random.normal(key, SHAPES[name], jnp.float32) * SHAPES[name][1] ** -0.5
        drawn[name] = (w * {"w_gate": 1.0, "w_up": bump(kh, FF, 4.0), "w_down": layers}[name]).astype(jnp.bfloat16)
    return drawn


def matmul(a, w):
    return jnp.dot(a, w, preferred_element_type=jnp.float32).astype(jnp.bfloat16)


def normed(h):
    wide = h.astype(jnp.float32)
    scale = lax.rsqrt(jnp.mean(wide**2, -1, keepdims=True) + 1e-6)
    return (wide * scale).astype(jnp.bfloat16)


def layer(h, w):
    a = normed(h)
    gate = jnp.dot(a, w["w_gate"], preferred_element_type=jnp.float32)
    up = jnp.dot(a, w["w_up"], preferred_element_type=jnp.float32)
    return h + matmul((jax.nn.silu(gate) * up).astype(jnp.bfloat16), w["w_down"])


def stack(weights, h):
    return lax.scan(lambda h, w: (layer(h, w), None), h, weights)[0]


def reference(x, dy, w_gate, w_up, w_down):
    weights = dict(zip(NAMES, (w_gate, w_up, w_down), strict=True))

    def take(so_far, sequence):
        h, by_y = sequence
        _, back = jax.vjp(stack, weights, h)
        by_weights, by_h = back(by_y)
        return jax.tree.map(lambda total, term: total + term.astype(jnp.float32), so_far, by_weights), by_h

    none_yet = {name: jnp.zeros(w.shape, jnp.float32) for name, w in weights.items()}
    by_weights, by_x = lax.scan(take, none_yet, (x, dy))
    return (by_x, *(by_weights[name].astype(jnp.bfloat16) for name in NAMES))
```

```python
import functools

import jax
import jax.numpy as jnp
from jax import lax
from jax.experimental import pallas as pl
from jax.experimental.pallas import tpu as pltpu
from jax.sharding import PartitionSpec as P

MESH = pl.DeviceIdType.MESH
f32, bf16 = jnp.float32, jnp.bfloat16

T, D, F, C = 2048, 896, 2304, 256
LAYERS, CHUNKS = 2, F // C
NX, NY, NZ, NS = 4, 4, 8, 8
RG, RD = D // NS, F // NS
PART = 42 * 16
PADDED = 44 * 16
QY, QZ = PADDED // NY, 32
TM = 512
TL = 256
NT = T // TL
PERIOD = CHUNKS + NT
LB, LC, LD, LE, LF = 1, 3, 4, 5, 6


def dot(a, b, ca=1, cb=0):
    return lax.dot_general(a, b, (((ca,), (cb,)), ((), ())), preferred_element_type=f32)


def normed(wide):
    scale = lax.rsqrt(jnp.mean(wide * wide, -1, keepdims=True) + 1e-6)
    return (wide * scale).astype(bf16)


def pack_kernel(wg, wu, wd, own):
    def gate_up(step, _):
        layer, i = step // 7, step % 7
        rows = pl.ds(pl.multiple_of(i * 16, 16), 16)
        for k, w in enumerate((wg, wu)):
            strip = w[layer, rows, :]
            for c in range(CHUNKS):
                for j in range(2):
                    parts = [strip[:, (9 * s + c) * 32 : (9 * s + c) * 32 + 32] for s in range(4 * j, 4 * j + 4)]
                    at = pl.ds(pl.multiple_of((k * 14 + j + i * 2) * 16, 16), 16)
                    own[layer * CHUNKS + c, at, :] = jnp.concatenate(parts, axis=1)
        return 0

    lax.fori_loop(0, 7 * LAYERS, gate_up, 0)

    def down(step, _):
        layer, c = step // CHUNKS, step % CHUNKS
        for i in range(2):
            strip = wd[layer, pl.ds(pl.multiple_of(c * 32 + i * 16, 16), 16), :]
            for j in range(7):
                own[step, pl.ds((28 + i * 7 + j) * 16, 16), :] = strip[:, j * 128 : j * 128 + 128]
        return 0

    lax.fori_loop(0, LAYERS * CHUNKS, down, 0)


def unpack_kernel(sums, og, ou, od):
    def gate_up(step, _):
        layer, i = step // 7, step % 7
        rows = pl.ds(pl.multiple_of(i * 16, 16), 16)
        for k, out in enumerate((og, ou)):
            for lane in range(18):
                parts = []
                for q in range(4 * lane, 4 * lane + 4):
                    s, c = q // 9, q % 9
                    at = pl.ds(pl.multiple_of((k * 14 + s // 4 + i * 2) * 16, 16), 16)
                    tile = sums[layer * CHUNKS + c, at, :]
                    parts.append(tile[:, s % 4 * 32 : s % 4 * 32 + 32])
                out[layer, rows, pl.ds(lane * 128, 128)] = jnp.concatenate(parts, axis=1)
        return 0

    lax.fori_loop(0, 7 * LAYERS, gate_up, 0)

    def down(step, _):
        layer, c = step // CHUNKS, step % CHUNKS
        for i in range(2):
            for j in range(7):
                od[layer, pl.ds(pl.multiple_of(c * 32 + i * 16, 16), 16), pl.ds(j * 128, 128)] = sums[
                    step, pl.ds((28 + i * 7 + j) * 16, 16), :
                ]
        return 0

    lax.fori_loop(0, LAYERS * CHUNKS, down, 0)


def kernel(
    own, x_in, dy_in,
    got, sums, dx_out,
    hx, dh, a, a_t, dh_t, wg, wu, wd, hid, dg, du, flat, xt,
    term, pair, x_out, x_got, y_out, y_got, z_out, z_got, z_sum, y_sum,
    g_send, g1_recv, g2_recv, g3_recv, load_sem, io_sem, xt_sem,
    pair_send, pair_recv, x_send, x_recv, y_send, y_recv, z_send, z_recv, zs_send, zs_recv, ys_send, ys_recv,
):
    s, r = lax.axis_index("s"), lax.axis_index("r")
    x, core, y, z = s // 2, s % 2, r // NZ, r % NZ

    def at(dx=0, dc=0, dy=0, dz=0):
        there = (y + dy) % NY * NZ + (z + dz) % NZ
        return (0, there, (x + dx) % NX * 2 + (core + dc) % 2)

    def shard(dx):
        return (x + dx) % NX * 2 + core

    def send(src, dst, send_sem, recv_sem, to):
        pltpu.make_async_remote_copy(
            src_ref=src, dst_ref=dst, send_sem=send_sem, recv_sem=recv_sem, device_id=to, device_id_type=MESH
        ).start()

    def wait(ref, sem):
        pltpu.make_async_copy(ref, ref, sem).wait()

    def rows(start, n):
        return pl.ds(pl.multiple_of(start, 16), n)

    def cols(c):
        return pl.ds(pl.multiple_of(c * C, C), C)

    def loop(n, body):
        lax.fori_loop(0, n, lambda i, _: (body(i), 0)[1], 0)

    get_x = pltpu.make_async_copy(x_in.at[0], hx, io_sem.at[0])
    get_dy = pltpu.make_async_copy(dy_in.at[0], dh, io_sem.at[1])
    get_x.start()
    get_dy.start()

    peers = [dict(dc=1)]
    peers += [dict(dx=i) for i in (1, 2, 3)] + [dict(dy=i) for i in (1, 2, 3)] + [dict(dz=i) for i in range(1, NZ)]
    barrier = pltpu.get_barrier_semaphore()
    for p in peers:
        pl.semaphore_signal(barrier, inc=1, device_id=at(**p), device_id_type=MESH)
    pl.semaphore_wait(barrier, len(peers))

    by_y, by_z = rows(y * 80, 80), rows(320 + z % 4 * 80, 80)

    def gather_1(ch):
        for dx in (1, 2, 3):
            for part in (by_y, by_z, pl.ds(640, 32)):
                send(own.at[ch, part], got.at[ch, s, part], g_send.at[ch], g1_recv.at[ch], at(dx=dx))

    def gather_2(ch):
        wait(got.at[ch, 0, pl.ds(0, 576)], g1_recv.at[ch])
        for dx in (1, 2, 3):
            here = shard(dx)

            def on(part, **to):
                part = got.at[ch, here, part]
                send(part, part, g_send.at[ch], g2_recv.at[ch], at(**to))

            on(by_z, dz=1)
            on(by_z, dz=-1)
            if dx == 1:
                on(by_z, dz=2)
            if dx == 2:
                on(rows(320 + z % 4 * 80, 48), dz=2)
                on(rows(368 + z % 4 * 80, 32), dz=-2)
            if dx == 3:
                on(by_z, dz=-2)
            for dy in (1, 2, 3):
                on(by_y, dy=dy)

    def gather_3(ch):
        wait(got.at[ch, pl.ds(0, 3), pl.ds(0, 480)], g2_recv.at[ch])
        send(own.at[ch], got.at[ch, s], g_send.at[ch], g3_recv.at[ch], at(dc=1))
        for dx in (1, 2, 3):
            part = got.at[ch, shard(dx)]
            send(part, part, g_send.at[ch], g3_recv.at[ch], at(dc=1))

    def load(ch):
        pltpu.make_async_copy(own.at[ch], flat.at[s], load_sem).start()
        for d in range(1, NS):
            other = (s + d) % NS
            pltpu.make_async_copy(got.at[ch, other], flat.at[other], load_sem).start()

    def arrived(ch):
        wait(got.at[ch, pl.ds(0, 4)], g3_recv.at[ch])

    def unpack(c):
        wait(flat, load_sem)

        def one(p):
            for i in range(7):
                for j in range(2):
                    there = (rows(p * RG + i * 16, 16), pl.ds(pl.multiple_of(c * C + j * 128, 128), 128))
                    wg[there] = flat[p, pl.ds((i * 2 + j) * 16, 16), :]
                    wu[there] = flat[p, pl.ds((14 + i * 2 + j) * 16, 16), :]
            for i in range(2):
                for j in range(7):
                    wd[rows(c * C + p * 32 + i * 16, 16), pl.ds(j * 128, 128)] = flat[p, pl.ds((28 + i * 7 + j) * 16, 16), :]

        loop(NS, one)

    def pump(ch):
        n = LAYERS * CHUNKS

        @pl.when(ch + 3 < n)
        def _():
            gather_2(ch + 3)

        @pl.when(ch + 2 < n)
        def _():
            gather_3(ch + 2)

        @pl.when(ch + 1 < n)
        def _():
            arrived(ch + 1)
            load(ch + 1)

    def add(out, *terms):
        out[...] = functools.reduce(lambda p, q: p + q, [t[...].astype(f32) for t in terms]).astype(bf16)

    def in_blocks(n, fn):
        loop(n // 176, lambda b: fn(rows(b * 176, 176)))

    def step_a(v):
        slot = v % 2
        for dx in range(NX):
            there = (x + dx) % NX
            send(term.at[slot, there * 2 + 1 - core], pair.at[slot, there], pair_send.at[slot], pair_recv.at[slot], at(dc=1))

    def step_b(v):
        slot, xs, xr = v % 2, v % 2, v % 4
        wait(pair.at[slot], pair_recv.at[slot])
        wait(pair.at[slot], pair_send.at[slot])
        for dx in (1, 2, 3, 0):
            there = (x + dx) % NX

            def block(part):
                out = x_out.at[xs, dx - 1, part] if dx else x_got.at[xr, 3, part]
                add(out, term.at[slot, there * 2 + core, part], pair.at[slot, there, part])

            in_blocks(PADDED, block)
            if dx:
                send(x_out.at[xs, dx - 1], x_got.at[xr, dx - 1], x_send.at[xs], x_recv.at[xr], at(dx=dx))

    def step_c(v):
        xs, xr, slot = v % 2, v % 4, v % 2
        wait(x_got.at[xr, pl.ds(0, 3)], x_recv.at[xr])
        wait(x_out.at[xs], x_send.at[xs])
        for dy in (1, 2, 3, 0):
            part = rows((y + dy) % NY * QY, QY)
            out = y_out.at[slot, dy - 1] if dy else y_got.at[slot, 3]
            add(out, *(x_got.at[xr, k, part] for k in (3, 0, 1, 2)))
            if dy:
                send(y_out.at[slot, dy - 1], y_got.at[slot, dy - 1], y_send.at[slot], y_recv.at[slot], at(dy=dy))

    def step_d(v):
        slot = v % 2
        wait(y_got.at[slot, pl.ds(0, 3)], y_recv.at[slot])
        wait(y_out.at[slot], y_send.at[slot])
        add(z_out.at[slot, pl.ds(0, QY)], *(y_got.at[slot, k] for k in (3, 0, 1, 2)))
        for dz in range(1, NZ):
            part = rows((z + dz) % NZ * QZ, QZ)
            send(z_out.at[slot, part], z_got.at[slot, dz - 1], z_send.at[slot], z_recv.at[slot], at(dz=dz))

    def step_e(v):
        slot = v % 2
        wait(z_got.at[slot], z_recv.at[slot])
        wait(z_got.at[slot], z_send.at[slot])
        mine = rows(z * QZ, QZ)
        add(z_sum.at[slot, mine], z_out.at[slot, mine], *(z_got.at[slot, k] for k in range(NZ - 1)))
        for dz in range(1, NZ):
            send(z_sum.at[slot, mine], z_sum.at[slot, mine], zs_send.at[slot], zs_recv.at[slot], at(dz=dz))

    def step_f(v):
        slot, ch = v % 2, chunk_of(v)
        wait(z_sum.at[slot, pl.ds(0, QZ * (NZ - 1))], zs_recv.at[slot])
        wait(z_sum.at[slot, pl.ds(0, QZ * (NZ - 1))], zs_send.at[slot])
        mine = rows(y * QY, QY)
        y_sum[ch] = z_sum[slot, pl.ds(0, QY), :]
        pltpu.make_async_copy(y_sum.at[ch], sums.at[ch, mine], ys_send.at[ch]).start()
        for dy in (1, 2, 3):
            send(y_sum.at[ch], sums.at[ch, mine], ys_send.at[ch], ys_recv.at[ch], at(dy=dy))

    def chunk_of(v):
        return (1 - v // PERIOD) * CHUNKS + v % PERIOD

    def tick(now):
        for lag, step in ((LF, step_f), (LE, step_e), (LD, step_d), (LC, step_c), (LB, step_b)):
            v = now - lag

            @pl.when((v >= 0) & (v < 2 * PERIOD) & (lax.rem(v + PERIOD, PERIOD) < CHUNKS))
            def _():
                step(v)

    loop(CHUNKS, gather_1)
    get_x.wait()

    def first_norm(m):
        part = rows(m * TL, TL)
        a[part, :] = normed(hx[part, :].astype(f32))

    loop(NT, first_norm)
    gather_2(0)
    gather_2(1)
    gather_3(0)
    gather_2(2)
    arrived(0)
    load(0)
    gather_3(1)

    def forward_half(c, half):
        for t in range(T // TM // 2):
            part = pl.ds(half * (T // 2) + t * TM, TM)
            gate = dot(a[part, :], wg[:, cols(c)])
            up = dot(a[part, :], wu[:, cols(c)])
            dg[part, cols(c)] = (jax.nn.silu(gate) * up).astype(bf16)

    def forward(c):
        unpack(c)
        gather_1(c + CHUNKS)
        forward_half(c, 0)
        pump(c)
        forward_half(c, 1)

    loop(CHUNKS, forward)
    get_dy.wait()

    def finish_forward(m):
        part = rows(m * TL, TL)
        lanes = pl.ds(pl.multiple_of(m * TL, TL), TL)
        out = dot(dg[part, :], wd[...]).astype(bf16)
        h = hx[part, :] + out
        hx[part, :] = h
        act = normed(h.astype(f32))
        a[part, :] = act
        a_t[:, lanes] = act.T
        dh_t[:, lanes] = dh[part, :].T

    loop(NT, finish_forward)

    def backward_half(c, half):
        for t in range(T // TM // 2):
            part = pl.ds(half * (T // 2) + t * TM, TM)
            gate = dot(a[part, :], wg[:, cols(c)])
            up = dot(a[part, :], wu[:, cols(c)])
            by_hid = dot(dh[part, :], wd[pl.ds(pl.multiple_of(c * C, C), C), :], 1, 1).astype(bf16).astype(f32)
            sig = jax.nn.sigmoid(gate)
            silu = gate * sig
            hid[part, :] = (silu * up).astype(bf16)
            dg[part, cols(c)] = (by_hid * up * (sig * (1 + gate * (1 - sig)))).astype(bf16)
            du[part, cols(c)] = (by_hid * silu).astype(bf16)

    def weight_grads(c, slot):
        for k, (left, right) in enumerate(((a_t, dg), (a_t, du), (dh_t, None))):
            out = dot(left[...], hid[...] if right is None else right[:, cols(c)])
            out = out.astype(bf16) if k < 2 else out.T.astype(bf16)
            up, wide = (7, 2) if k < 2 else (2, 7)
            for p in range(NS):
                for i in range(up):
                    for j in range(wide):
                        term[slot, p, pl.ds((k * 14 + i * wide + j) * 16, 16), :] = out[
                            (p * up + i) * 16 : (p * up + i) * 16 + 16, j * 128 : j * 128 + 128
                        ]

    for slot in range(2):
        for p in range(NS):
            term[slot, p, pl.ds(PART, PADDED - PART), :] = jnp.zeros((PADDED - PART, 128), bf16)
        z_out[slot, pl.ds(QY, NZ * QZ - QY), :] = jnp.zeros((NZ * QZ - QY, 128), bf16)

    def fetch(m, slot):
        return pltpu.make_async_copy(x_in.at[0, rows(m * TL, TL)], xt.at[slot], xt_sem.at[slot])

    def backward(turn):
        def first(c):
            v = turn * PERIOD + c
            ch = (1 - turn) * CHUNKS + c
            unpack(c)
            backward_half(c, 0)

            @pl.when(turn == 0)
            def _():
                pump(ch)

            @pl.when((turn == 0) & (c == CHUNKS - 1))
            def _():
                load(0)

            @pl.when((turn == 1) & (c < CHUNKS - 1))
            def _():
                load(c + 1)

            backward_half(c, 1)
            tick(v)
            weight_grads(c, v % 2)
            step_a(v)

        loop(CHUNKS, first)
        fetch(0, 0).start()

        def second(m):
            part = rows(m * TL, TL)
            lanes = pl.ds(pl.multiple_of(m * TL, TL), TL)
            fetch(m, m % 2).wait()

            @pl.when(m + 1 < NT)
            def _():
                fetch(m + 1, (m + 1) % 2).start()

            by_a = dot(dg[part, :], wg[...], 1, 1) + dot(du[part, :], wu[...], 1, 1)
            by_a = by_a.astype(bf16).astype(f32)
            wide = hx[part, :].astype(f32)
            scale = lax.rsqrt(jnp.mean(wide * wide, -1, keepdims=True) + 1e-6)
            along = jnp.mean(by_a * wide, -1, keepdims=True)
            by_h = (by_a * scale - wide * (scale * scale * scale * along)).astype(bf16)
            by_h = dh[part, :] + by_h
            dh[part, :] = by_h
            dh_t[:, lanes] = by_h.T
            h = xt[m % 2]
            hx[part, :] = h
            act = normed(h.astype(f32))
            a[part, :] = act
            a_t[:, lanes] = act.T
            tick(turn * PERIOD + CHUNKS + m)

        loop(NT, second)

    loop(2, backward)

    put_dx = pltpu.make_async_copy(dh, dx_out.at[0], io_sem.at[0])
    put_dx.start()

    def finish(ch):
        wait(sums.at[ch, pl.ds(0, 3 * QY)], ys_recv.at[ch])
        wait(sums.at[ch], ys_send.at[ch])
        wait(got.at[ch, pl.ds(0, 7)], g_send.at[ch])

    loop(LAYERS * CHUNKS, finish)
    put_dx.wait()


def solution(mesh):
    def step(x, dy, w_gate, w_up, w_down):
        anywhere = pl.BlockSpec(memory_space=pl.ANY)
        n = LAYERS * CHUNKS
        shape = jax.ShapeDtypeStruct
        own = pl.pallas_call(
            pack_kernel, out_shape=shape((n, PART, 128), bf16), compiler_params=pltpu.CompilerParams(vmem_limit_bytes=40 * 2**20)
        )(w_gate, w_up, w_down)
        vmem = lambda *dims, dtype=bf16: pltpu.VMEM(dims, dtype)
        dma = lambda *dims: pltpu.SemaphoreType.DMA(dims)
        _, sums, by_x = pl.pallas_call(
            kernel,
            out_shape=(shape((n, NS, PART, 128), bf16), shape((n, PADDED, 128), bf16), shape((1, T, D), bf16)),
            in_specs=[anywhere] * 3,
            out_specs=(anywhere,) * 3,
            scratch_shapes=[
                vmem(T, D), vmem(T, D), vmem(T, D), vmem(D, T), vmem(D, T),
                vmem(D, F), vmem(D, F), vmem(F, D), vmem(T, C), vmem(T, F), vmem(T, F),
                vmem(NS, PART, 128), vmem(2, TL, D),
                vmem(2, NS, PADDED, 128), vmem(2, NX, PADDED, 128), vmem(2, 3, PADDED, 128), vmem(4, 4, PADDED, 128),
                vmem(2, 3, QY, 128), vmem(2, 4, QY, 128), vmem(2, NZ * QZ, 128), vmem(2, NZ - 1, QZ, 128),
                vmem(2, NZ * QZ, 128), vmem(n, QY, 128),
                dma(n), dma(n), dma(n), dma(n), pltpu.SemaphoreType.DMA, dma(2), dma(2),
                dma(2), dma(2), dma(2), dma(4), dma(2), dma(2), dma(2), dma(2), dma(2), dma(2), dma(n), dma(n),
            ],
            compiler_params=pltpu.CompilerParams(collective_id=0, has_side_effects=True, vmem_limit_bytes=67043328),
        )(own, x, dy)
        grads = pl.pallas_call(
            unpack_kernel,
            out_shape=(shape((LAYERS, RG, F), bf16), shape((LAYERS, RG, F), bf16), shape((LAYERS, RD, D), bf16)),
            compiler_params=pltpu.CompilerParams(vmem_limit_bytes=40 * 2**20),
        )(sums)
        return (by_x, *grads)

    states, cut = P(("rep", "r", "s"), None, None), P(None, "s", None)
    return jax.shard_map(
        step,
        mesh=mesh,
        in_specs=(states, states) + (cut,) * 3,
        out_specs=(states,) + (P("rep", "s", None),) * 3,
        check_vma=False,
    )
```

```python
import functools

import jax
import jax.numpy as jnp
from jax import lax
from jax.experimental import pallas as pl
from jax.experimental.pallas import tpu as pltpu
from jax.sharding import PartitionSpec as P

MESH = pl.DeviceIdType.MESH
f32, bf16 = jnp.float32, jnp.bfloat16

T, D, F, C = 2048, 896, 2304, 256
LAYERS, CHUNKS = 2, F // C
N = LAYERS * CHUNKS
NX, NY, NZ, NS = 4, 4, 8, 8
RG, RD = D // NS, F // NS
PART = 42 * 16
PADDED = 44 * 16
QY, QZ = PADDED // NY, 32
QA = 112
QB = QY - QA
TM = 512
TL = 256
NT = T // TL
PERIOD = CHUNKS + NT // 2
LB, LC, LD, LE, LF, LG = 1, 3, 5, 7, 9, 10


def dot(a, b, ca=1, cb=0):
    return lax.dot_general(a, b, (((ca,), (cb,)), ((), ())), preferred_element_type=f32)


def normed(wide):
    scale = lax.rsqrt(jnp.mean(wide * wide, -1, keepdims=True) + 1e-6)
    return (wide * scale).astype(bf16)


def mod(a, b):
    return a % b if isinstance(a, int) else lax.rem(a, b)


def div(a, b):
    return a // b if isinstance(a, int) else lax.div(a, b)


def in2(v):
    return mod(v, 2)


def in4(v):
    return mod(v, 4)


def rows(start, n):
    return pl.ds(pl.multiple_of(start, 16), n)


def cols(c):
    return pl.ds(pl.multiple_of(c * C, C), C)


def loop(n, body):
    lax.fori_loop(0, n, lambda i, _: (body(i), 0)[1], 0)


def wait(ref, sem):
    pltpu.make_async_copy(ref, ref, sem).wait()


def unpack_kernel(sums_in, dx_in, dx_out, og_out, ou_out, od_out, sums, dx, og, ou, od, in_sem, dx_sem, out_sem):
    for layer in (1, 0):
        half = pl.ds(layer * CHUNKS, CHUNKS)
        pltpu.make_async_copy(sums_in.at[half], sums.at[half], in_sem.at[layer]).start()
    moves = []
    for k in range(4):
        part = pl.ds(k * (T // 4), T // 4)
        pltpu.make_async_copy(dx_in.at[0, part], dx.at[part], dx_sem.at[k]).start()
        moves.append((dx_in.at[0, part], dx.at[part], dx_out.at[0, part], dx_sem.at[k]))
    for src, mid, dst, sem in moves:
        pltpu.make_async_copy(src, mid, sem).wait()
        pltpu.make_async_copy(mid, dst, sem).start()
    for layer in (1, 0):
        wait(sums.at[pl.ds(layer * CHUNKS, CHUNKS)], in_sem.at[layer])

        def gate_up(i):
            for k, out in enumerate((og, ou)):
                for lane in range(18):
                    parts = []
                    for q in range(4 * lane, 4 * lane + 4):
                        s, c = q // 9, q % 9
                        at = rows((k * 14 + s // 4 + i * 2) * 16, 16)
                        parts.append(sums[layer * CHUNKS + c, at, :][:, s % 4 * 32 : s % 4 * 32 + 32])
                    out[layer, rows(i * 16, 16), pl.ds(lane * 128, 128)] = jnp.concatenate(parts, axis=1)

        loop(7, gate_up)

        def down(c):
            for i in range(2):
                for j in range(7):
                    there = (layer, rows(c * 32 + i * 16, 16), pl.ds(j * 128, 128))
                    od[there] = sums[layer * CHUNKS + c, pl.ds((28 + i * 7 + j) * 16, 16), :]

        loop(CHUNKS, down)
        for k, (mid, out) in enumerate(((og, og_out), (ou, ou_out), (od, od_out))):
            pltpu.make_async_copy(mid.at[layer], out.at[layer], out_sem.at[layer * 3 + k]).start()
    for layer in (1, 0):
        for k, (mid, out) in enumerate(((og, og_out), (ou, ou_out), (od, od_out))):
            pltpu.make_async_copy(mid.at[layer], out.at[layer], out_sem.at[layer * 3 + k]).wait()
    for _, mid, dst, sem in moves:
        pltpu.make_async_copy(mid, dst, sem).wait()


def kernel(
    x_in, dy_in, wg_in, wu_in, wd_in,
    own, got, sums, dx_out, kept, kept_hid,
    hx, dh, a, a_t, dh_t, wg, wu, wd, hid, dg, du, keep, flat, xt,
    term, pair, both, x_got, y_got, a_out, b_out, a_got, b_got, z_out, z_got, z_sum, y_sum,
    w_sem, own_sem, fence_sem, g1_send, g_send, g1_recv, g2_recv, g3_recv, load_sem, io_sem, xt_sem, keep_sem, hid_sem,
    pair_send, pair_recv, x_send, x_recv, y_send, y_recv, a_send, a_recv, b_send, b_recv,
    z_send, z_recv, zs_send, zs_recv, ys_send, ys_recv,
):
    s, r = lax.axis_index("s"), lax.axis_index("r")
    x, core, y, z = div(s, 2), mod(s, 2), div(r, NZ), mod(r, NZ)

    def at(dx=0, dc=0, dy=0, dz=0):
        there = mod(y + dy, NY) * NZ + mod(z + dz, NZ)
        return (0, there, mod(x + dx, NX) * 2 + mod(core + dc, 2))

    def shard(dx):
        return mod(x + dx, NX) * 2 + core

    def send(src, dst, send_sem, recv_sem, to):
        pltpu.make_async_remote_copy(
            src_ref=src, dst_ref=dst, send_sem=send_sem, recv_sem=recv_sem, device_id=to, device_id_type=MESH
        ).start()

    def get_weights(layer):
        for k, w in enumerate((wg_in, wu_in)):
            there = du.at[pl.ds((layer * 2 + k) * RG, RG)]
            pltpu.make_async_copy(w.at[layer], there, w_sem.at[layer]).start()
        there = dh_t.at[pl.ds(layer * RD, RD), pl.ds(0, D)]
        pltpu.make_async_copy(wd_in.at[layer], there, w_sem.at[layer + 2]).start()

    get_weights(0)
    get_x = pltpu.make_async_copy(x_in.at[0], hx, io_sem.at[0])
    get_dy = pltpu.make_async_copy(dy_in.at[0], dh, io_sem.at[1])

    peers = [dict(dc=1)]
    peers += [dict(dx=i) for i in (1, 2, 3)] + [dict(dy=i) for i in (1, 2, 3)] + [dict(dz=i) for i in range(1, NZ)]
    barrier = pltpu.get_barrier_semaphore()
    for p in peers:
        pl.semaphore_signal(barrier, inc=1, device_id=at(**p), device_id_type=MESH)

    def staged(ch):
        return term.at[div(ch, NS), mod(ch, NS)] if ch < 2 * NS else pair.at[0, ch - 2 * NS]

    def pack(layer):
        wait(du.at[pl.ds(0, 2 * RG)], w_sem.at[layer])
        wait(dh_t.at[pl.ds(0, RD), pl.ds(0, D)], w_sem.at[layer + 2])

        def gate_up(i):
            for k in range(2):
                strip = du[rows((layer * 2 + k) * RG + i * 16, 16), :]
                for c in range(CHUNKS):
                    for j in range(2):
                        there = staged(layer * CHUNKS + c)
                        for q in range(4):
                            old = (9 * (4 * j + q) + c) * 32
                            there[rows((k * 14 + j + i * 2) * 16, 16), pl.ds(q * 32, 32)] = strip[:, old : old + 32]

        loop(7, gate_up)
        for c in range(CHUNKS):
            there = staged(layer * CHUNKS + c)
            for i in range(2):
                for j in range(7):
                    tile = dh_t[pl.ds(layer * RD + c * 32 + i * 16, 16), pl.ds(j * 128, 128)]
                    there[pl.ds((28 + i * 7 + j) * 16, 16), :] = tile
            pltpu.make_async_copy(there.at[pl.ds(0, PART)], own.at[layer * CHUNKS + c], own_sem).start()

    def packed():
        wait(own.at[pl.ds(0, CHUNKS)], own_sem)

    by_y, by_z = rows(y * 80, 80), rows(320 + mod(z, 4) * 80, 80)

    def gather_1(ch, part_of, sem):
        for dx in (1, 2, 3):
            for part in (by_y, by_z, pl.ds(640, 32)):
                send(part_of.at[part], got.at[ch, s, part], sem, g1_recv.at[ch], at(dx=dx))

    def gather_2(ch):
        wait(got.at[ch, 0, pl.ds(0, 576)], g1_recv.at[ch])
        for dx in (1, 2, 3):
            here = shard(dx)

            def on(part, **to):
                part = got.at[ch, here, part]
                send(part, part, g_send.at[ch], g2_recv.at[ch], at(**to))

            on(by_z, dz=1)
            on(by_z, dz=NZ - 1)
            if dx == 1:
                on(by_z, dz=2)
            if dx == 2:
                on(rows(320 + mod(z, 4) * 80, 48), dz=2)
                on(rows(368 + mod(z, 4) * 80, 32), dz=NZ - 2)
            if dx == 3:
                on(by_z, dz=NZ - 2)
            for dy in (1, 2, 3):
                on(by_y, dy=dy)

    def gather_3(ch):
        wait(got.at[ch, pl.ds(0, 3), pl.ds(0, 480)], g2_recv.at[ch])
        send(own.at[ch], got.at[ch, s], g_send.at[ch], g3_recv.at[ch], at(dc=1))
        for dx in (1, 2, 3):
            part = got.at[ch, shard(dx)]
            send(part, part, g_send.at[ch], g3_recv.at[ch], at(dc=1))

    def load(ch):
        pltpu.make_async_copy(own.at[ch], flat.at[s], load_sem).start()
        for d in range(1, NS):
            other = mod(s + d, NS)
            pltpu.make_async_copy(got.at[ch, other], flat.at[other], load_sem).start()

    def arrived(ch):
        wait(got.at[ch, pl.ds(0, 4)], g3_recv.at[ch])

    def loaded():
        wait(flat, load_sem)

    def unpack_one(c, p):
        for i in range(7):
            for j in range(2):
                there = (rows(p * RG + i * 16, 16), pl.ds(pl.multiple_of(c * C + j * 128, 128), 128))
                wg[there] = flat[p, pl.ds((i * 2 + j) * 16, 16), :]
                wu[there] = flat[p, pl.ds((14 + i * 2 + j) * 16, 16), :]
        for i in range(2):
            for j in range(7):
                wd[rows(p * 32 + i * 16, 16), pl.ds(j * 128, 128)] = flat[p, pl.ds((28 + i * 7 + j) * 16, 16), :]

    def unpack(c):
        loop(NS, lambda p: unpack_one(c, p))

    def pump(ch):
        pl.when(ch + 3 < N)(lambda: gather_2(ch + 3))
        pl.when(ch + 2 < N)(lambda: gather_3(ch + 2))

        @pl.when(ch + 1 < N)
        def _():
            arrived(ch + 1)
            load(ch + 1)

    def fence():
        pl.semaphore_signal(fence_sem, 1)
        pl.semaphore_wait(fence_sem, 1)

    def total(*terms):
        return functools.reduce(lambda p, q: p + q, [t.astype(f32) for t in terms]).astype(bf16)

    def step_a(v):
        slot = in2(v)
        for dx in range(NX):
            there = mod(x + dx, NX)
            send(term.at[slot, there * 2 + 1 - core], pair.at[slot, there], pair_send.at[slot], pair_recv.at[slot], at(dc=1))

    def wait_b(v):
        wait(pair.at[in2(v)], pair_recv.at[in2(v)])
        wait(pair.at[in2(v)], pair_send.at[in2(v)])

    def add_b(v, each):
        def one(k):
            i, part = div(k, NY), rows(mod(k, NY) * QY, QY)
            both[in2(v), i, mod(k, NY)] = total(term[in2(v), i * 2 + core, part, :], pair[in2(v), i, part, :])

        each(NX * NY, one)

    def send_b(v):
        for d in (1, 2, 3):
            src = both.at[in2(v), mod(x + d, NX), :, pl.ds(0, QA)]
            send(src, x_got.at[in4(v), d - 1], x_send.at[in2(v)], x_recv.at[in4(v)], at(dx=d))
            src = both.at[in2(v), :, mod(y + d, NY), pl.ds(QA, QB)]
            send(src, y_got.at[in4(v), d - 1], y_send.at[in2(v)], y_recv.at[in4(v)], at(dy=d))

    def wait_c(v):
        wait(x_got.at[in4(v)], x_recv.at[in4(v)])
        wait(y_got.at[in4(v)], y_recv.at[in4(v)])
        wait(x_got.at[in4(v)], x_send.at[in2(v)])
        wait(y_got.at[in4(v)], y_send.at[in2(v)])

    def add_c(v, each):
        for d in range(4):
            there = mod(y + d, NY)
            out = total(both[in2(v), x, there, pl.ds(0, QA), :], *(x_got[in4(v), k, there] for k in range(3)))
            if d:
                a_out[in2(v), d - 1] = out
            else:
                a_got[in4(v), 3] = out
            there = mod(x + d, NX)
            out = total(both[in2(v), there, y, pl.ds(QA, QB), :], *(y_got[in4(v), k, there] for k in range(3)))
            if d:
                b_out[in2(v), d - 1] = out
            else:
                b_got[in4(v), 3] = out

    def send_c(v):
        for d in (1, 2, 3):
            send(a_out.at[in2(v), d - 1], a_got.at[in4(v), d - 1], a_send.at[in4(v)], a_recv.at[in4(v)], at(dy=d))
            send(b_out.at[in2(v), d - 1], b_got.at[in4(v), d - 1], b_send.at[in4(v)], b_recv.at[in4(v)], at(dx=d))

    def wait_d(v):
        wait(a_out.at[in2(v)], a_recv.at[in4(v)])
        wait(b_out.at[in2(v)], b_recv.at[in4(v)])
        wait(a_out.at[in2(v)], a_send.at[in4(v)])
        wait(b_out.at[in2(v)], b_send.at[in4(v)])

    def add_d(v, each):
        z_out[in4(v), pl.ds(0, QA), :] = total(*(a_got[in4(v), k] for k in (3, 0, 1, 2)))
        z_out[in4(v), pl.ds(QA, QB), :] = total(*(b_got[in4(v), k] for k in (3, 0, 1, 2)))

    def send_d(v):
        for d in range(1, NZ):
            src = z_out.at[in4(v), rows(mod(z + d, NZ) * QZ, QZ)]
            send(src, z_got.at[in4(v), d - 1], z_send.at[in4(v)], z_recv.at[in4(v)], at(dz=d))

    def wait_e(v):
        wait(z_got.at[in4(v)], z_recv.at[in4(v)])
        wait(z_got.at[in4(v)], z_send.at[in4(v)])

    def add_e(v, each):
        mine = rows(z * QZ, QZ)
        z_sum[in4(v), mine, :] = total(z_out[in4(v), mine, :], *(z_got[in4(v), k] for k in range(NZ - 1)))

    def send_e(v):
        mine = z_sum.at[in4(v), rows(z * QZ, QZ)]
        for d in range(1, NZ):
            send(mine, mine, zs_send.at[in4(v)], zs_recv.at[in4(v)], at(dz=d))

    def wait_f(v):
        wait(z_sum.at[in4(v), pl.ds(0, QZ * (NZ - 1))], zs_recv.at[in4(v)])
        wait(z_sum.at[in4(v), pl.ds(0, QZ * (NZ - 1))], zs_send.at[in4(v)])

    def send_f(v):
        ch, mine = (1 - div(v, PERIOD)) * CHUNKS + mod(v, PERIOD), rows(y * QY, QY)
        y_sum[in2(v)] = z_sum[in4(v), pl.ds(0, QY), :]
        pltpu.make_async_copy(y_sum.at[in2(v)], sums.at[ch, mine], ys_send.at[in4(v)]).start()
        for d in (1, 2, 3):
            send(y_sum.at[in2(v)], sums.at[ch, mine], ys_send.at[in4(v)], ys_recv.at[ch], at(dy=d))

    def wait_g(v):
        wait(sums.at[0], ys_send.at[in4(v)])

    def send_g(v):
        pass

    steps = (
        (LG, wait_g, None, send_g),
        (LF, wait_f, None, send_f),
        (LE, wait_e, add_e, send_e),
        (LD, wait_d, add_d, send_d),
        (LC, wait_c, add_c, send_c),
        (LB, wait_b, add_b, send_b),
    )

    def real(v):
        return (v >= 0) & (v < 2 * PERIOD) & (lax.rem(v + PERIOD, PERIOD) < CHUNKS)

    def waits(now, steps=steps):
        for lag, first, _, _ in steps:
            pl.when(real(now - lag))(lambda: first(now - lag))

    def adds(now, steps=steps):
        for lag, _, add, _ in steps:
            if add:
                pl.when(real(now - lag))(lambda: add(now - lag, loop))

    def unrolled(n, body):
        for k in range(n):
            body(k)

    def sends(now):
        for lag, _, _, last in steps:
            pl.when(real(now - lag))(lambda: last(now - lag))

    def tick(now):
        waits(now)
        adds(now)
        sends(now)

    pack(0)
    get_x.start()
    get_weights(1)
    pl.semaphore_wait(barrier, len(peers))
    for ch in range(CHUNKS):
        gather_1(ch, staged(ch), g1_send.at[0])
    get_x.wait()

    def first_norm(m):
        part = rows(m * TL, TL)
        a[part, :] = normed(hx[part, :].astype(f32))

    loop(NT, first_norm)
    gather_2(0)
    gather_2(1)
    packed()
    pack(1)
    get_dy.start()
    gather_3(0)
    gather_2(2)
    packed()
    arrived(0)
    load(0)
    gather_3(1)

    def keeping(c, half):
        part = pl.ds(half * (T // 2), T // 2)
        return pltpu.make_async_copy(keep.at[:, part], kept.at[c, :, part], keep_sem.at[half])

    def forward_half(c, half):
        for t in range(T // TM // 2):
            part = pl.ds(half * (T // 2) + t * TM, TM)
            gate = dot(a[part, :], wg[:, cols(c)])
            up = dot(a[part, :], wu[:, cols(c)])
            sig = jax.nn.sigmoid(gate)
            silu = gate * sig
            dg[part, cols(c)] = (silu * up).astype(bf16)
            keep[0, part, :] = silu
            keep[1, part, :] = up * (sig * (1 + gate * (1 - sig)))

    def forward(c):
        loaded()
        unpack(c)
        gather_1(c + CHUNKS, own.at[c + CHUNKS], g1_send.at[1])
        pl.when(c >= 1)(lambda: keeping(c, 0).wait())
        du[pl.ds(0, D), cols(c)] = wd[...].T
        forward_half(c, 0)
        keeping(c, 0).start()
        pump(c)
        fence()
        pl.when(c >= 1)(lambda: keeping(c, 1).wait())
        forward_half(c, 1)
        keeping(c, 1).start()

    loop(CHUNKS, forward)
    get_dy.wait()

    loop(CHUNKS, lambda c: pltpu.make_async_copy(dg.at[:, cols(c)], kept_hid.at[c], hid_sem).start())

    def finish_forward(m):
        part = rows(m * TL, TL)
        lanes = pl.ds(pl.multiple_of(m * TL, TL), TL)
        out = dot(dg[part, :], du[pl.ds(0, D), :], 1, 1).astype(bf16)
        h = hx[part, :] + out
        hx[part, :] = h
        act = normed(h.astype(f32))
        a[part, :] = act
        a_t[:, lanes] = act.T
        dh_t[:, lanes] = dh[part, :].T

    loop(NT, finish_forward)
    keeping(0, 0).wait()
    keeping(0, 1).wait()
    wait(dg, hid_sem)

    def fetch_kept(c):
        return (
            pltpu.make_async_copy(kept.at[c], keep, keep_sem.at[0]),
            pltpu.make_async_copy(kept_hid.at[c], hid.at[in2(c)], hid_sem),
        )

    def by_hid(part):
        return dot(dh[part, :], wd[...], 1, 1).astype(bf16).astype(f32)

    def backward_half(c, half):
        for t in range(T // TM // 2):
            part = pl.ds(half * (T // 2) + t * TM, TM)
            gate = dot(a[part, :], wg[:, cols(c)])
            up = dot(a[part, :], wu[:, cols(c)])
            by = by_hid(part)
            sig = jax.nn.sigmoid(gate)
            silu = gate * sig
            hid[1, part, :] = (silu * up).astype(bf16)
            dg[part, cols(c)] = (by * (up * (sig * (1 + gate * (1 - sig))))).astype(bf16)
            du[part, cols(c)] = (by * silu).astype(bf16)

    def backward_kept(c):
        for t in range(T // TM):
            part = pl.ds(t * TM, TM)
            by = by_hid(part)
            dg[part, cols(c)] = (by * keep[1, part, :]).astype(bf16)
            du[part, cols(c)] = (by * keep[0, part, :]).astype(bf16)

    def weight_grads(c, slot, hid_slot):
        for k, (left, right) in enumerate(((a_t, dg), (a_t, du), (dh_t, None))):
            out = dot(left[...], hid[hid_slot] if right is None else right[:, cols(c)])
            out = out.astype(bf16) if k < 2 else out.T.astype(bf16)
            up, wide = (7, 2) if k < 2 else (2, 7)
            for p in range(NS):
                for i in range(up):
                    for j in range(wide):
                        term[slot, p, pl.ds((k * 14 + i * wide + j) * 16, 16), :] = out[
                            (p * up + i) * 16 : (p * up + i) * 16 + 16, j * 128 : j * 128 + 128
                        ]

    wait(got.at[pl.ds(0, CHUNKS), 0, pl.ds(0, 576)], g1_send.at[0])
    for slot in range(4):
        z_out[slot, pl.ds(QY, NZ * QZ - QY), :] = jnp.zeros((NZ * QZ - QY, 128), bf16)
    for slot in range(2):
        for p in range(NS):
            term[slot, p, pl.ds(PART, PADDED - PART), :] = jnp.zeros((PADDED - PART, 128), bf16)

    def gradients(turn, c, hid_slot):
        v = turn * PERIOD + c
        beside = steps[:-1] if turn else steps
        waits(v, beside)
        pl.when(c < CHUNKS - 1)(loaded)
        adds(v, steps[:-1])
        if not turn:
            add_b(v + 1, unrolled)
        for p in range(NS):
            unpack_one(c + 1 - div(c + 1, CHUNKS), p)
        weight_grads(c, in2(v), hid_slot)
        if turn:

            @pl.when(c >= 1)
            def _():
                wait_b(v - 1)
                add_b(v - 1, loop)
        sends(v)
        step_a(v)

    def fetch(m):
        return pltpu.make_async_copy(x_in.at[0, rows(m * TL, TL)], xt.at[in2(m)], xt_sem.at[in2(m)])

    def back_through_norm(turn, m):
        part = rows(m * TL, TL)
        by_a = dot(dg[part, :], wg[...], 1, 1) + dot(du[part, :], wu[...], 1, 1)
        by_a = by_a.astype(bf16).astype(f32)
        wide = hx[part, :].astype(f32)
        scale = lax.rsqrt(jnp.mean(wide * wide, -1, keepdims=True) + 1e-6)
        along = jnp.mean(by_a * wide, -1, keepdims=True)
        by_h = (by_a * scale - wide * (scale * scale * scale * along)).astype(bf16)
        by_h = dh[part, :] + by_h
        dh[part, :] = by_h
        return by_h

    loaded()
    unpack(0)
    for copy in fetch_kept(0):
        copy.start()

    def first_1(c):
        backward_half(c, 0)
        pump(CHUNKS + c)
        fence()
        backward_half(c, 1)
        gradients(0, c, 1)

    loop(CHUNKS, first_1)
    load(0)
    fetch(0).start()

    def second_1(m):
        lanes = pl.ds(pl.multiple_of(m * TL, TL), TL)
        fetch(m).wait()
        pl.when(m + 1 < NT)(lambda: fetch(m + 1).start())
        by_h = back_through_norm(0, m)
        dh_t[:, lanes] = by_h.T
        h = xt[in2(m)]
        hx[rows(m * TL, TL), :] = h
        act = normed(h.astype(f32))
        a_t[:, lanes] = act.T
        pl.when(in2(m) == 1)(lambda: tick(CHUNKS + div(m, 2)))

    loop(NT, second_1)

    loaded()
    unpack(0)

    def first_0(c):
        pl.when(c < CHUNKS - 1)(lambda: load(c + 1))
        for copy in fetch_kept(c):
            copy.wait()
        backward_kept(c)

        @pl.when(c < CHUNKS - 1)
        def _():
            for copy in fetch_kept(c + 1):
                copy.start()

        gradients(1, c, mod(c, 2))

    loop(CHUNKS, first_0)

    def second_0(m):
        back_through_norm(1, m)
        part = rows(m * TL, TL)
        pltpu.make_async_copy(dh.at[part], dx_out.at[0, part], io_sem.at[0]).start()
        loop(2, lambda i: pl.when((in2(m) == 1) & (m + i >= 2))(lambda: tick(PERIOD + CHUNKS - 2 + m + i)))

    loop(NT, second_0)

    loop(LG - NT + 1, lambda i: tick(PERIOD + CHUNKS + NT - 1 + i))

    def finish(ch):
        wait(sums.at[ch, pl.ds(0, 3 * QY)], ys_recv.at[ch])
        wait(sums.at[pl.ds(0, 6), pl.ds(0, 688)], g_send.at[ch])

    loop(N, finish)
    wait(got.at[pl.ds(0, CHUNKS), 0, pl.ds(0, 576)], g1_send.at[1])
    wait(dh, io_sem.at[0])


def solution(mesh):
    def step(x, dy, w_gate, w_up, w_down):
        anywhere = pl.BlockSpec(memory_space=pl.ANY)
        shape = jax.ShapeDtypeStruct
        vmem = lambda *dims, dtype=bf16: pltpu.VMEM(dims, dtype)
        dma = lambda *dims: pltpu.SemaphoreType.DMA(dims)
        one = pltpu.SemaphoreType.DMA
        _, _, sums, by_x, _, _ = pl.pallas_call(
            kernel,
            out_shape=(
                shape((N, PART, 128), bf16), shape((N, NS, PART, 128), bf16), shape((N, PADDED, 128), bf16), shape((1, T, D), bf16),
                shape((CHUNKS, 2, T, C), f32), shape((CHUNKS, T, C), bf16),
            ),
            in_specs=[anywhere] * 5,
            out_specs=(anywhere,) * 6,
            scratch_shapes=[
                vmem(T, D), vmem(T, D), vmem(T, D), vmem(D, T), vmem(D, T),
                vmem(D, F), vmem(D, F), vmem(C, D), vmem(2, T, C), vmem(T, F), vmem(T, F), vmem(2, T, C, dtype=f32),
                vmem(NS, PART, 128), vmem(2, TL, D),
                vmem(2, NS, PADDED, 128), vmem(2, NX, PADDED, 128), vmem(2, NX, NY, QY, 128),
                vmem(4, 3, NY, QA, 128), vmem(4, 3, NX, QB, 128),
                vmem(2, 3, QA, 128), vmem(2, 3, QB, 128), vmem(4, 4, QA, 128), vmem(4, 4, QB, 128),
                vmem(4, NZ * QZ, 128), vmem(4, NZ - 1, QZ, 128), vmem(4, NZ * QZ, 128), vmem(2, QY, 128),
                dma(4), one, pltpu.SemaphoreType.REGULAR, dma(2), dma(N), dma(N), dma(N), dma(N), one, dma(2), dma(2), dma(2), one,
                *[dma(4)] * 15, dma(N),
            ],
            compiler_params=pltpu.CompilerParams(collective_id=0, has_side_effects=True, vmem_limit_bytes=67043328),
        )(x, dy, w_gate, w_up, w_down)
        return pl.pallas_call(
            unpack_kernel,
            out_shape=(
                shape((1, T, D), bf16), shape((LAYERS, RG, F), bf16), shape((LAYERS, RG, F), bf16), shape((LAYERS, RD, D), bf16)
            ),
            in_specs=[anywhere] * 2,
            out_specs=(anywhere,) * 4,
            scratch_shapes=[
                vmem(N, PADDED, 128), vmem(T, D), vmem(LAYERS, RG, F), vmem(LAYERS, RG, F), vmem(LAYERS, RD, D),
                dma(2), dma(4), dma(6),
            ],
            compiler_params=pltpu.CompilerParams(vmem_limit_bytes=67043328),
        )(sums, by_x)

    states, cut = P(("rep", "r", "s"), None, None), P(None, "s", None)
    return jax.shard_map(
        step,
        mesh=mesh,
        in_specs=(states, states) + (cut,) * 3,
        out_specs=(states,) + (P("rep", "s", None),) * 3,
        check_vma=False,
    )
```

```python
import functools

import jax
import jax.numpy as jnp
from jax import lax
from jax.experimental import pallas as pl
from jax.experimental.pallas import tpu as pltpu
from jax.sharding import PartitionSpec as P

MESH = pl.DeviceIdType.MESH
f32, bf16 = jnp.float32, jnp.bfloat16

T, D, F, C = 2048, 896, 2304, 256
LAYERS, CHUNKS = 2, F // C
N = LAYERS * CHUNKS
NX, NY, NZ, NS = 4, 4, 8, 8
RG, RD = D // NS, F // NS
PART = 42 * 16
PADDED = 44 * 16
QY, QZ = PADDED // NY, 32
QA = 112
QB = QY - QA
TM = 512
TL = 256
NT = T // TL
PERIOD = CHUNKS + NT // 2
LB, LC, LD, LE, LF, LG = 1, 3, 5, 7, 9, 10


def dot(a, b, ca=1, cb=0):
    return lax.dot_general(a, b, (((ca,), (cb,)), ((), ())), preferred_element_type=f32)


def normed(wide):
    scale = lax.rsqrt(jnp.mean(wide * wide, -1, keepdims=True) + 1e-6)
    return (wide * scale).astype(bf16)


def mod(a, b):
    return a % b if isinstance(a, int) else lax.rem(a, b)


def div(a, b):
    return a // b if isinstance(a, int) else lax.div(a, b)


def in2(v):
    return mod(v, 2)


def in4(v):
    return mod(v, 4)


def rows(start, n):
    return pl.ds(pl.multiple_of(start, 16), n)


def cols(c):
    return pl.ds(pl.multiple_of(c * C, C), C)


def loop(n, body):
    lax.fori_loop(0, n, lambda i, _: (body(i), 0)[1], 0)


def wait(ref, sem):
    pltpu.make_async_copy(ref, ref, sem).wait()


def unpack_kernel(sums_in, dx_in, dx_out, og_out, ou_out, od_out, sums, dx, og, ou, od, in_sem, dx_sem, out_sem):
    for layer in (1, 0):
        half = pl.ds(layer * CHUNKS, CHUNKS)
        pltpu.make_async_copy(sums_in.at[half], sums.at[half], in_sem.at[layer]).start()
    moves = []
    for k in range(4):
        part = pl.ds(k * (T // 4), T // 4)
        pltpu.make_async_copy(dx_in.at[0, part], dx.at[part], dx_sem.at[k]).start()
        moves.append((dx_in.at[0, part], dx.at[part], dx_out.at[0, part], dx_sem.at[k]))
    for src, mid, dst, sem in moves:
        pltpu.make_async_copy(src, mid, sem).wait()
        pltpu.make_async_copy(mid, dst, sem).start()
    for layer in (1, 0):
        wait(sums.at[pl.ds(layer * CHUNKS, CHUNKS)], in_sem.at[layer])

        def gate_up(i):
            for k, out in enumerate((og, ou)):
                for lane in range(18):
                    parts = []
                    for q in range(4 * lane, 4 * lane + 4):
                        s, c = q // 9, q % 9
                        at = rows((k * 14 + s // 4 + i * 2) * 16, 16)
                        parts.append(sums[layer * CHUNKS + c, at, :][:, s % 4 * 32 : s % 4 * 32 + 32])
                    out[layer, rows(i * 16, 16), pl.ds(lane * 128, 128)] = jnp.concatenate(parts, axis=1)

        loop(7, gate_up)

        def down(c):
            for i in range(2):
                for j in range(7):
                    there = (layer, rows(c * 32 + i * 16, 16), pl.ds(j * 128, 128))
                    od[there] = sums[layer * CHUNKS + c, pl.ds((28 + i * 7 + j) * 16, 16), :]

        loop(CHUNKS, down)
        for k, (mid, out) in enumerate(((og, og_out), (ou, ou_out), (od, od_out))):
            pltpu.make_async_copy(mid.at[layer], out.at[layer], out_sem.at[layer * 3 + k]).start()
    for layer in (1, 0):
        for k, (mid, out) in enumerate(((og, og_out), (ou, ou_out), (od, od_out))):
            pltpu.make_async_copy(mid.at[layer], out.at[layer], out_sem.at[layer * 3 + k]).wait()
    for _, mid, dst, sem in moves:
        pltpu.make_async_copy(mid, dst, sem).wait()


def kernel(
    x_in, dy_in, wg_in, wu_in, wd_in,
    own, got, sums, dx_out, kept, kept_hid,
    hx, dh, a, a_t, dh_t, wg, wu, wd, hid, dg, du, keep, flat, xt,
    term, pair, both, x_got, y_got, a_out, b_out, a_got, b_got, z_out, z_got, z_sum, y_sum,
    w_sem, own_sem, fence_sem, g1_send, g_send, g1_recv, g2_recv, g3_recv, load_sem, io_sem, xt_sem, keep_sem, hid_sem,
    pair_send, pair_recv, x_send, x_recv, y_send, y_recv, a_send, a_recv, b_send, b_recv,
    z_send, z_recv, zs_send, zs_recv, ys_send, ys_recv,
):
    s, r = lax.axis_index("s"), lax.axis_index("r")
    x, core, y, z = div(s, 2), mod(s, 2), div(r, NZ), mod(r, NZ)

    def at(dx=0, dc=0, dy=0, dz=0):
        there = mod(y + dy, NY) * NZ + mod(z + dz, NZ)
        return (0, there, mod(x + dx, NX) * 2 + mod(core + dc, 2))

    def shard(dx):
        return mod(x + dx, NX) * 2 + core

    def send(src, dst, send_sem, recv_sem, to):
        pltpu.make_async_remote_copy(
            src_ref=src, dst_ref=dst, send_sem=send_sem, recv_sem=recv_sem, device_id=to, device_id_type=MESH
        ).start()

    def get_weights(layer):
        for k, w in enumerate((wg_in, wu_in)):
            there = du.at[pl.ds((layer * 2 + k) * RG, RG)]
            pltpu.make_async_copy(w.at[layer], there, w_sem.at[layer]).start()
        there = dh_t.at[pl.ds(layer * RD, RD), pl.ds(0, D)]
        pltpu.make_async_copy(wd_in.at[layer], there, w_sem.at[layer + 2]).start()

    get_weights(0)
    get_x = pltpu.make_async_copy(x_in.at[0], hx, io_sem.at[0])
    get_dy = pltpu.make_async_copy(dy_in.at[0], dh, io_sem.at[1])

    peers = [dict(dc=1)]
    peers += [dict(dx=i) for i in (1, 2, 3)] + [dict(dy=i) for i in (1, 2, 3)] + [dict(dz=i) for i in range(1, NZ)]
    barrier = pltpu.get_barrier_semaphore()
    for p in peers:
        pl.semaphore_signal(barrier, inc=1, device_id=at(**p), device_id_type=MESH)

    def staged(ch):
        return term.at[div(ch, NS), mod(ch, NS)] if ch < 2 * NS else pair.at[0, ch - 2 * NS]

    def pack(layer):
        wait(du.at[pl.ds(0, 2 * RG)], w_sem.at[layer])
        wait(dh_t.at[pl.ds(0, RD), pl.ds(0, D)], w_sem.at[layer + 2])

        def gate_up(i):
            for k in range(2):
                strip = du[rows((layer * 2 + k) * RG + i * 16, 16), :]
                for c in range(CHUNKS):
                    for j in range(2):
                        there = staged(layer * CHUNKS + c)
                        for q in range(4):
                            old = (9 * (4 * j + q) + c) * 32
                            there[rows((k * 14 + j + i * 2) * 16, 16), pl.ds(q * 32, 32)] = strip[:, old : old + 32]

        loop(7, gate_up)
        for c in range(CHUNKS):
            there = staged(layer * CHUNKS + c)
            for i in range(2):
                for j in range(7):
                    tile = dh_t[pl.ds(layer * RD + c * 32 + i * 16, 16), pl.ds(j * 128, 128)]
                    there[pl.ds((28 + i * 7 + j) * 16, 16), :] = tile
            pltpu.make_async_copy(there.at[pl.ds(0, PART)], own.at[layer * CHUNKS + c], own_sem).start()

    def packed():
        wait(own.at[pl.ds(0, CHUNKS)], own_sem)

    by_y, by_z = rows(y * 80, 80), rows(320 + mod(z, 4) * 80, 80)

    def gather_1(ch, part_of, sem):
        for dx in (1, 2, 3):
            for part in (by_y, by_z, pl.ds(640, 32)):
                send(part_of.at[part], got.at[ch, s, part], sem, g1_recv.at[ch], at(dx=dx))

    def gather_2(ch):
        wait(got.at[ch, 0, pl.ds(0, 576)], g1_recv.at[ch])
        for dx in (1, 2, 3):
            here = shard(dx)

            def on(part, **to):
                part = got.at[ch, here, part]
                send(part, part, g_send.at[ch], g2_recv.at[ch], at(**to))

            on(by_z, dz=1)
            on(by_z, dz=NZ - 1)
            if dx == 1:
                on(by_z, dz=2)
            if dx == 2:
                on(rows(320 + mod(z, 4) * 80, 48), dz=2)
                on(rows(368 + mod(z, 4) * 80, 32), dz=NZ - 2)
            if dx == 3:
                on(by_z, dz=NZ - 2)
            for dy in (1, 2, 3):
                on(by_y, dy=dy)

    def gather_3(ch):
        wait(got.at[ch, pl.ds(0, 3), pl.ds(0, 480)], g2_recv.at[ch])
        send(own.at[ch], got.at[ch, s], g_send.at[ch], g3_recv.at[ch], at(dc=1))
        for dx in (1, 2, 3):
            part = got.at[ch, shard(dx)]
            send(part, part, g_send.at[ch], g3_recv.at[ch], at(dc=1))

    def load(ch):
        pltpu.make_async_copy(own.at[ch], flat.at[s], load_sem).start()
        for d in range(1, NS):
            other = mod(s + d, NS)
            pltpu.make_async_copy(got.at[ch, other], flat.at[other], load_sem).start()

    def arrived(ch):
        wait(got.at[ch, pl.ds(0, 4)], g3_recv.at[ch])

    def loaded():
        wait(flat, load_sem)

    def unpack_one(c, p):
        for i in range(7):
            for j in range(2):
                there = (rows(p * RG + i * 16, 16), pl.ds(pl.multiple_of(c * C + j * 128, 128), 128))
                wg[there] = flat[p, pl.ds((i * 2 + j) * 16, 16), :]
                wu[there] = flat[p, pl.ds((14 + i * 2 + j) * 16, 16), :]
        for i in range(2):
            for j in range(7):
                wd[rows(p * 32 + i * 16, 16), pl.ds(j * 128, 128)] = flat[p, pl.ds((28 + i * 7 + j) * 16, 16), :]

    def unpack(c):
        loop(NS, lambda p: unpack_one(c, p))

    def pump(ch):
        pl.when(ch + 3 < N)(lambda: gather_2(ch + 3))
        pl.when(ch + 2 < N)(lambda: gather_3(ch + 2))

        @pl.when(ch + 1 < N)
        def _():
            arrived(ch + 1)
            load(ch + 1)

    def fence():
        pl.semaphore_signal(fence_sem, 1)
        pl.semaphore_wait(fence_sem, 1)

    def total(*terms):
        return functools.reduce(lambda p, q: p + q, [t.astype(f32) for t in terms]).astype(bf16)

    def step_a(v):
        slot = in2(v)
        for dx in range(NX):
            there = mod(x + dx, NX)
            send(term.at[slot, there * 2 + 1 - core], pair.at[slot, there], pair_send.at[slot], pair_recv.at[slot], at(dc=1))

    def wait_b(v):
        wait(pair.at[in2(v)], pair_recv.at[in2(v)])
        wait(pair.at[in2(v)], pair_send.at[in2(v)])

    def add_b(v, each):
        def one(k):
            i, part = div(k, NY), rows(mod(k, NY) * QY, QY)
            both[in2(v), i, mod(k, NY)] = total(term[in2(v), i * 2 + core, part, :], pair[in2(v), i, part, :])

        each(NX * NY, one)

    def send_b(v):
        for d in (1, 2, 3):
            src = both.at[in2(v), mod(x + d, NX), :, pl.ds(0, QA)]
            send(src, x_got.at[in4(v), d - 1], x_send.at[in2(v)], x_recv.at[in4(v)], at(dx=d))
            src = both.at[in2(v), :, mod(y + d, NY), pl.ds(QA, QB)]
            send(src, y_got.at[in4(v), d - 1], y_send.at[in2(v)], y_recv.at[in4(v)], at(dy=d))

    def wait_c(v):
        wait(x_got.at[in4(v)], x_recv.at[in4(v)])
        wait(y_got.at[in4(v)], y_recv.at[in4(v)])
        wait(x_got.at[in4(v)], x_send.at[in2(v)])
        wait(y_got.at[in4(v)], y_send.at[in2(v)])

    def add_c(v, each):
        for d in range(4):
            there = mod(y + d, NY)
            out = total(both[in2(v), x, there, pl.ds(0, QA), :], *(x_got[in4(v), k, there] for k in range(3)))
            if d:
                a_out[in2(v), d - 1] = out
            else:
                a_got[in4(v), 3] = out
            there = mod(x + d, NX)
            out = total(both[in2(v), there, y, pl.ds(QA, QB), :], *(y_got[in4(v), k, there] for k in range(3)))
            if d:
                b_out[in2(v), d - 1] = out
            else:
                b_got[in4(v), 3] = out

    def send_c(v):
        for d in (1, 2, 3):
            send(a_out.at[in2(v), d - 1], a_got.at[in4(v), d - 1], a_send.at[in4(v)], a_recv.at[in4(v)], at(dy=d))
            send(b_out.at[in2(v), d - 1], b_got.at[in4(v), d - 1], b_send.at[in4(v)], b_recv.at[in4(v)], at(dx=d))

    def wait_d(v):
        wait(a_out.at[in2(v)], a_recv.at[in4(v)])
        wait(b_out.at[in2(v)], b_recv.at[in4(v)])
        wait(a_out.at[in2(v)], a_send.at[in4(v)])
        wait(b_out.at[in2(v)], b_send.at[in4(v)])

    def add_d(v, each):
        z_out[in4(v), pl.ds(0, QA), :] = total(*(a_got[in4(v), k] for k in (3, 0, 1, 2)))
        z_out[in4(v), pl.ds(QA, QB), :] = total(*(b_got[in4(v), k] for k in (3, 0, 1, 2)))

    def send_d(v):
        for d in range(1, NZ):
            src = z_out.at[in4(v), rows(mod(z + d, NZ) * QZ, QZ)]
            send(src, z_got.at[in4(v), d - 1], z_send.at[in4(v)], z_recv.at[in4(v)], at(dz=d))

    def wait_e(v):
        wait(z_got.at[in4(v)], z_recv.at[in4(v)])
        wait(z_got.at[in4(v)], z_send.at[in4(v)])

    def add_e(v, each):
        mine = rows(z * QZ, QZ)
        z_sum[in4(v), mine, :] = total(z_out[in4(v), mine, :], *(z_got[in4(v), k] for k in range(NZ - 1)))

    def send_e(v):
        mine = z_sum.at[in4(v), rows(z * QZ, QZ)]
        for d in range(1, NZ):
            send(mine, mine, zs_send.at[in4(v)], zs_recv.at[in4(v)], at(dz=d))

    def wait_f(v):
        wait(z_sum.at[in4(v), pl.ds(0, QZ * (NZ - 1))], zs_recv.at[in4(v)])
        wait(z_sum.at[in4(v), pl.ds(0, QZ * (NZ - 1))], zs_send.at[in4(v)])

    def send_f(v):
        ch, mine = (1 - div(v, PERIOD)) * CHUNKS + mod(v, PERIOD), rows(y * QY, QY)
        y_sum[in2(v)] = z_sum[in4(v), pl.ds(0, QY), :]
        pltpu.make_async_copy(y_sum.at[in2(v)], sums.at[ch, mine], ys_send.at[in4(v)]).start()
        for d in (1, 2, 3):
            send(y_sum.at[in2(v)], sums.at[ch, mine], ys_send.at[in4(v)], ys_recv.at[ch], at(dy=d))

    def wait_g(v):
        wait(sums.at[0], ys_send.at[in4(v)])

    def send_g(v):
        pass

    steps = (
        (LG, wait_g, None, send_g),
        (LF, wait_f, None, send_f),
        (LE, wait_e, add_e, send_e),
        (LD, wait_d, add_d, send_d),
        (LC, wait_c, add_c, send_c),
        (LB, wait_b, add_b, send_b),
    )

    def real(v):
        return (v >= 0) & (v < 2 * PERIOD) & (lax.rem(v + PERIOD, PERIOD) < CHUNKS)

    def waits(now, steps=steps):
        for lag, first, _, _ in steps:
            pl.when(real(now - lag))(lambda: first(now - lag))

    def adds(now, steps=steps):
        for lag, _, add, _ in steps:
            if add:
                pl.when(real(now - lag))(lambda: add(now - lag, loop))

    def unrolled(n, body):
        for k in range(n):
            body(k)

    def sends(now, steps=steps):
        for lag, _, _, last in steps:
            pl.when(real(now - lag))(lambda: last(now - lag))

    def tick(now):
        waits(now)
        adds(now)
        sends(now)

    pack(0)
    get_x.start()
    get_weights(1)
    pl.semaphore_wait(barrier, len(peers))
    for ch in range(CHUNKS):
        gather_1(ch, staged(ch), g1_send.at[0])
    gather_2(0)
    get_x.wait()

    def first_norm(m):
        part = rows(m * TL, TL)
        a[part, :] = normed(hx[part, :].astype(f32))

    loop(NT, first_norm)
    gather_2(1)
    packed()
    pack(1)
    get_dy.start()
    gather_3(0)
    gather_2(2)
    packed()
    arrived(0)
    load(0)
    gather_3(1)

    def keeping(c, half):
        part = pl.ds(half * (T // 2), T // 2)
        return pltpu.make_async_copy(keep.at[:, part], kept.at[c, :, part], keep_sem.at[half])

    def forward_half(c, half):
        for t in range(T // TM // 2):
            part = pl.ds(half * (T // 2) + t * TM, TM)
            gate = dot(a[part, :], wg[:, cols(c)])
            up = dot(a[part, :], wu[:, cols(c)])
            sig = jax.nn.sigmoid(gate)
            silu = gate * sig
            dg[part, cols(c)] = (silu * up).astype(bf16)
            keep[0, part, :] = silu
            keep[1, part, :] = up * (sig * (1 + gate * (1 - sig)))

    def forward(c):
        loaded()
        unpack(c)
        gather_1(c + CHUNKS, own.at[c + CHUNKS], g1_send.at[1])
        pl.when(c >= 1)(lambda: keeping(c, 0).wait())
        du[pl.ds(0, D), cols(c)] = wd[...].T
        forward_half(c, 0)
        keeping(c, 0).start()
        pump(c)
        fence()
        pl.when(c >= 1)(lambda: keeping(c, 1).wait())
        forward_half(c, 1)
        keeping(c, 1).start()

    loop(CHUNKS, forward)
    get_dy.wait()

    loop(CHUNKS, lambda c: pltpu.make_async_copy(dg.at[:, cols(c)], kept_hid.at[c], hid_sem).start())

    def finish_forward(m):
        part = rows(m * TL, TL)
        lanes = pl.ds(pl.multiple_of(m * TL, TL), TL)
        out = dot(dg[part, :], du[pl.ds(0, D), :], 1, 1).astype(bf16)
        h = hx[part, :] + out
        hx[part, :] = h
        act = normed(h.astype(f32))
        a[part, :] = act
        a_t[:, lanes] = act.T
        dh_t[:, lanes] = dh[part, :].T

    loop(NT, finish_forward)
    keeping(0, 0).wait()
    keeping(0, 1).wait()
    wait(dg, hid_sem)

    def fetch_kept(c):
        return (
            pltpu.make_async_copy(kept.at[c], keep, keep_sem.at[0]),
            pltpu.make_async_copy(kept_hid.at[c], hid.at[in2(c)], hid_sem),
        )

    def by_hid(part):
        return dot(dh[part, :], wd[...], 1, 1).astype(bf16).astype(f32)

    def backward_half(c, half):
        for t in range(T // TM // 2):
            part = pl.ds(half * (T // 2) + t * TM, TM)
            gate = dot(a[part, :], wg[:, cols(c)])
            up = dot(a[part, :], wu[:, cols(c)])
            by = by_hid(part)
            sig = jax.nn.sigmoid(gate)
            silu = gate * sig
            hid[1, part, :] = (silu * up).astype(bf16)
            dg[part, cols(c)] = (by * (up * (sig * (1 + gate * (1 - sig))))).astype(bf16)
            du[part, cols(c)] = (by * silu).astype(bf16)

    def backward_kept(c):
        for t in range(T // TM):
            part = pl.ds(t * TM, TM)
            by = by_hid(part)
            dg[part, cols(c)] = (by * keep[1, part, :]).astype(bf16)
            du[part, cols(c)] = (by * keep[0, part, :]).astype(bf16)

    def weight_grads(c, slot, hid_slot):
        for k, (left, right) in enumerate(((a_t, dg), (a_t, du), (dh_t, None))):
            out = dot(left[...], hid[hid_slot] if right is None else right[:, cols(c)])
            out = out.astype(bf16) if k < 2 else out.T.astype(bf16)
            up, wide = (7, 2) if k < 2 else (2, 7)
            for p in range(NS):
                for i in range(up):
                    for j in range(wide):
                        term[slot, p, pl.ds((k * 14 + i * wide + j) * 16, 16), :] = out[
                            (p * up + i) * 16 : (p * up + i) * 16 + 16, j * 128 : j * 128 + 128
                        ]

    wait(got.at[pl.ds(0, CHUNKS), 0, pl.ds(0, 576)], g1_send.at[0])
    for slot in range(4):
        z_out[slot, pl.ds(QY, NZ * QZ - QY), :] = jnp.zeros((NZ * QZ - QY, 128), bf16)
    for slot in range(2):
        for p in range(NS):
            term[slot, p, pl.ds(PART, PADDED - PART), :] = jnp.zeros((PADDED - PART, 128), bf16)

    def gradients(turn, c, hid_slot):
        v = turn * PERIOD + c
        beside = steps[:-1] if turn else steps
        waits(v, beside)
        pl.when(c < CHUNKS - 1)(loaded)
        adds(v, steps[:-1])
        sends(v, steps[:-1])
        fence()
        if not turn:
            add_b(v + 1, unrolled)
        for p in range(NS):
            unpack_one(c + 1 - div(c + 1, CHUNKS), p)
        weight_grads(c, in2(v), hid_slot)
        if turn:

            @pl.when(c >= 1)
            def _():
                wait_b(v - 1)
                add_b(v - 1, loop)
        sends(v, steps[-1:])
        step_a(v)

    def fetch(m):
        return pltpu.make_async_copy(x_in.at[0, rows(m * TL, TL)], xt.at[in2(m)], xt_sem.at[in2(m)])

    def back_through_norm(turn, m):
        part = rows(m * TL, TL)
        by_a = dot(dg[part, :], wg[...], 1, 1) + dot(du[part, :], wu[...], 1, 1)
        by_a = by_a.astype(bf16).astype(f32)
        wide = hx[part, :].astype(f32)
        scale = lax.rsqrt(jnp.mean(wide * wide, -1, keepdims=True) + 1e-6)
        along = jnp.mean(by_a * wide, -1, keepdims=True)
        by_h = (by_a * scale - wide * (scale * scale * scale * along)).astype(bf16)
        by_h = dh[part, :] + by_h
        dh[part, :] = by_h
        return by_h

    loaded()
    unpack(0)
    for copy in fetch_kept(0):
        copy.start()

    def first_1(c):
        backward_half(c, 0)
        pump(CHUNKS + c)
        fence()
        backward_half(c, 1)
        gradients(0, c, 1)

    loop(CHUNKS, first_1)
    load(0)
    fetch(0).start()

    def second_1(m):
        lanes = pl.ds(pl.multiple_of(m * TL, TL), TL)
        fetch(m).wait()
        pl.when(m + 1 < NT)(lambda: fetch(m + 1).start())
        by_h = back_through_norm(0, m)
        dh_t[:, lanes] = by_h.T
        h = xt[in2(m)]
        hx[rows(m * TL, TL), :] = h
        act = normed(h.astype(f32))
        a_t[:, lanes] = act.T
        pl.when(in2(m) == 0)(lambda: tick(CHUNKS + div(m, 2)))

    loop(NT, second_1)

    loaded()
    unpack(0)

    def first_0(c):
        pl.when(c < CHUNKS - 1)(lambda: load(c + 1))
        for copy in fetch_kept(c):
            copy.wait()
        backward_kept(c)

        @pl.when(c < CHUNKS - 1)
        def _():
            for copy in fetch_kept(c + 1):
                copy.start()

        gradients(1, c, mod(c, 2))

    loop(CHUNKS, first_0)

    def second_0(m):
        back_through_norm(1, m)
        part = rows(m * TL, TL)
        pltpu.make_async_copy(dh.at[part], dx_out.at[0, part], io_sem.at[0]).start()
        loop(2, lambda i: pl.when((in2(m) == 0) & (m + i >= 1))(lambda: tick(PERIOD + CHUNKS - 1 + m + i)))

    loop(NT, second_0)

    loop(LG - NT + 1, lambda i: tick(PERIOD + CHUNKS + NT - 1 + i))

    def finish(ch):
        wait(sums.at[ch, pl.ds(0, 3 * QY)], ys_recv.at[ch])
        wait(sums.at[pl.ds(0, 6), pl.ds(0, 688)], g_send.at[ch])

    loop(N, finish)
    wait(got.at[pl.ds(0, CHUNKS), 0, pl.ds(0, 576)], g1_send.at[1])
    wait(dh, io_sem.at[0])


def solution(mesh):
    def step(x, dy, w_gate, w_up, w_down):
        anywhere = pl.BlockSpec(memory_space=pl.ANY)
        shape = jax.ShapeDtypeStruct
        vmem = lambda *dims, dtype=bf16: pltpu.VMEM(dims, dtype)
        dma = lambda *dims: pltpu.SemaphoreType.DMA(dims)
        one = pltpu.SemaphoreType.DMA
        _, _, sums, by_x, _, _ = pl.pallas_call(
            kernel,
            out_shape=(
                shape((N, PART, 128), bf16), shape((N, NS, PART, 128), bf16), shape((N, PADDED, 128), bf16), shape((1, T, D), bf16),
                shape((CHUNKS, 2, T, C), f32), shape((CHUNKS, T, C), bf16),
            ),
            in_specs=[anywhere] * 5,
            out_specs=(anywhere,) * 6,
            scratch_shapes=[
                vmem(T, D), vmem(T, D), vmem(T, D), vmem(D, T), vmem(D, T),
                vmem(D, F), vmem(D, F), vmem(C, D), vmem(2, T, C), vmem(T, F), vmem(T, F), vmem(2, T, C, dtype=f32),
                vmem(NS, PART, 128), vmem(2, TL, D),
                vmem(2, NS, PADDED, 128), vmem(2, NX, PADDED, 128), vmem(2, NX, NY, QY, 128),
                vmem(4, 3, NY, QA, 128), vmem(4, 3, NX, QB, 128),
                vmem(2, 3, QA, 128), vmem(2, 3, QB, 128), vmem(4, 4, QA, 128), vmem(4, 4, QB, 128),
                vmem(4, NZ * QZ, 128), vmem(4, NZ - 1, QZ, 128), vmem(4, NZ * QZ, 128), vmem(2, QY, 128),
                dma(4), one, pltpu.SemaphoreType.REGULAR, dma(2), dma(N), dma(N), dma(N), dma(N), one, dma(2), dma(2), dma(2), one,
                *[dma(4)] * 15, dma(N),
            ],
            compiler_params=pltpu.CompilerParams(collective_id=0, has_side_effects=True, vmem_limit_bytes=67043328),
        )(x, dy, w_gate, w_up, w_down)
        return pl.pallas_call(
            unpack_kernel,
            out_shape=(
                shape((1, T, D), bf16), shape((LAYERS, RG, F), bf16), shape((LAYERS, RG, F), bf16), shape((LAYERS, RD, D), bf16)
            ),
            in_specs=[anywhere] * 2,
            out_specs=(anywhere,) * 4,
            scratch_shapes=[
                vmem(N, PADDED, 128), vmem(T, D), vmem(LAYERS, RG, F), vmem(LAYERS, RG, F), vmem(LAYERS, RD, D),
                dma(2), dma(4), dma(6),
            ],
            compiler_params=pltpu.CompilerParams(vmem_limit_bytes=67043328),
        )(sums, by_x)

    states, cut = P(("rep", "r", "s"), None, None), P(None, "s", None)
    return jax.shard_map(
        step,
        mesh=mesh,
        in_specs=(states, states) + (cut,) * 3,
        out_specs=(states,) + (P("rep", "s", None),) * 3,
        check_vma=False,
    )
```
